32 devices in a mesh: angle: 4 (over z), pos: 8 (over y, x, core).
Axes of the slice: x: 2, y: 2, z: 4, core: 2. Of those that a mesh axis runs over, the one named last changes fastest.
Arguments:
- amplitude: float32 [4, 32, 128, 128], P('angle', 'pos'), may hold values from 0 to 2.5
- offsets: int32 [4, 32, 2], P('angle', 'pos'), may hold values from 0 to 896, as said below
- probe_field: float32 [2, 128, 128], replicated, may hold values from -5 to 5
- object_field: float32 [4, 2, 1024, 1024], P('angle', None, 'pos'), may hold values from -5 to 5
- interp_index: int32 [4, 2, 1024], replicated, may hold values from 0 to 1022
- interp_weight: float32 [4, 2, 1024], replicated, may hold values from 0 to 1
Outputs:
- new_object: float32 [4, 2, 1024, 1024], P('angle', None, 'pos')
- new_probe: float32 [2, 128, 128], replicated
- recon: float32 [8, 128, 2, 1024], P('pos', 'angle')
The draws below stay inside these ranges and needn't reach their ends.
Inputs may be any that keep to these rules, and one draw needn't show every extreme that they name: For position j, offsets[a, j, 0] = max(0, min(896, (j // 4) * 128 - 128 // 2 + u)) with 0 <= u < 128; offsets[a, j, 1] lies in 0 to 896.
All inputs are finite; a program needn't handle non-finite values.
Results may differ from the reference program's by a relative error of at most 0.00007.
Values sent between devices are 32-bit elements; how exact they have to be, the bound alone decides.
No kernel may reach another device: no remote copies, remote signals or barrier semaphores. Data moves between devices by JAX's collectives and lax.ppermute only.
A program may use at most 64 MiB of HBM per device.

```python
import math
import jax
import jax.numpy as jnp
from jax import lax

NOBJ = 1024
PATCH = 128
POS_DEV = 4
ZWIN = 2
ANGLES = 4
POSITIONS = 32
BAND = 128
N_POS = 8


def draw_offsets(key, part):
    key_rows = jax.random.fold_in(key, 11)
    key_cols = jax.random.fold_in(key, 12)
    owners = jnp.arange(POSITIONS, dtype=jnp.int32) // POS_DEV
    base = owners * BAND - PATCH // 2
    shifts = jax.random.randint(key_rows, (ANGLES, POSITIONS), 0, BAND, dtype=jnp.int32)
    first_rows = jnp.clip(base[None, :] + shifts, 0, NOBJ - PATCH)
    first_cols = jax.random.randint(key_cols, (ANGLES, POSITIONS), 0, NOBJ - PATCH + 1, dtype=jnp.int32)
    return jnp.stack([first_rows, first_cols], axis=-1).astype(jnp.int32)


def with_ends(array, own_key, low, high):
    longest = array.shape.index(max(array.shape))
    spots = []
    for shift in (0, 1):
        where = [jax.random.randint(jax.random.fold_in(own_key, axis), (), 0, length) for axis, length in enumerate(array.shape)]
        where[longest] = (where[longest] + shift) % array.shape[longest]
        spots.append(tuple(where))
    return array.at[spots[0]].set(low).at[spots[1]].set(high)


def block_scale(rng, dims, pieces, smallest, largest):
    factor_of, own = 1.0, jax.random.fold_in(rng, 6)
    for position, blocks in pieces:
        steps = jnp.exp(jax.random.uniform(jax.random.fold_in(own, position), (blocks,), jnp.float32, smallest / len(pieces), largest / len(pieces)))
        factor_of = factor_of * jnp.repeat(steps, dims[position] // blocks).reshape([-1 if axis == position else 1 for axis in range(len(dims))])
    return factor_of


def bell_draw(key, extent, scale, bound, split=(), kind=jnp.bfloat16):
    values = jax.random.normal(key, extent, jnp.float32) * scale
    if len(split) > 0:
        values = block_scale(key, extent, split, -0.22, 0.18) * values
    return jnp.clip(values, min=-bound, max=bound).astype(kind)


def setup_inputs(seed: int = 0) -> dict:
    seeds = jax.random.split(jax.random.key(seed), 7)
    amplitude = jnp.clip(2.5 * jax.random.uniform(seeds[0], (ANGLES, POSITIONS, PATCH, PATCH), jnp.float32) ** block_scale(seeds[0], (ANGLES, POSITIONS, PATCH, PATCH), ((0, 4), (1, 8)), -0.2, 0.2), 0.0, 2.5)
    offsets = draw_offsets(jax.random.fold_in(seeds[6], 71), 0)
    probe_field = bell_draw(seeds[2], (2, PATCH, PATCH), 0.8, 5.0, (), jnp.float32)
    object_field = bell_draw(seeds[3], (ANGLES, 2, NOBJ, NOBJ), 0.8, 5.0, ((0, 4), (2, 8)), jnp.float32)
    interp_index = with_ends(jax.random.randint(seeds[4], (ANGLES, ZWIN, NOBJ), 0, NOBJ - 1), jax.random.fold_in(seeds[4], 1), 0, (NOBJ - 1) - 1).astype(jnp.int32)
    interp_weight = jnp.clip(jax.random.uniform(seeds[5], (ANGLES, ZWIN, NOBJ), jnp.float32, 0.0, 1.0), 0.0, 1.0)
    return dict(amplitude=amplitude, offsets=offsets, probe_field=probe_field, object_field=object_field, interp_index=interp_index, interp_weight=interp_weight)


def ramp_matrix(length):
    ramp = jnp.arange(length, dtype=jnp.int32)
    differ = ramp[:, None] - ramp[None, :]
    spread = differ.astype(jnp.float32)
    squared = jnp.maximum(spread * spread, 1.0)
    odd_terms = jnp.where(differ % 2 != 0, -1.0 / (math.pi * math.pi * squared), 0.0)
    return jnp.where(differ == 0, 0.25, odd_terms).astype(jnp.float32)


def reference(amplitude, offsets, probe_field, object_field, interp_index, interp_weight):
    probe_c = lax.complex(probe_field[0], probe_field[1])
    power = probe_field[0] * probe_field[0] + probe_field[1] * probe_field[1]

    def one_angle(inputs):
        amps, places, layer = inputs
        field = lax.complex(layer[0], layer[1])

        def take_patch(place):
            return lax.dynamic_slice(field, (place[0], place[1]), (PATCH, PATCH))

        patches = jax.vmap(take_patch)(places)
        exit_wave = probe_c * patches
        spectrum = jnp.fft.fft2(exit_wave, norm="ortho")
        magnitude = jnp.abs(spectrum)
        fixed = spectrum * (amps / jnp.maximum(magnitude, 0.5))
        change = jnp.fft.ifft2(fixed, norm="ortho") - exit_wave
        contrib = jnp.conj(probe_c) * change
        numer = jnp.sum(jnp.conj(patches) * change, axis=0)
        denom = jnp.sum(jnp.real(patches) ** 2 + jnp.imag(patches) ** 2, axis=0)
        stacked = jnp.stack([jnp.real(contrib), jnp.imag(contrib), jnp.broadcast_to(power, contrib.shape)], axis=1)

        def accumulate(count, total):
            start = (jnp.int32(0), places[count, 0], places[count, 1])
            current = lax.dynamic_slice(total, start, (3, PATCH, PATCH))
            return lax.dynamic_update_slice(total, current + stacked[count], start)

        total = lax.fori_loop(0, POSITIONS, accumulate, jnp.zeros((3, NOBJ, NOBJ), jnp.float32))
        updated = layer + total[:2] / (total[2] + 1.0)
        return updated, jnp.stack([jnp.real(numer), jnp.imag(numer)]), denom

    new_object, numers, denoms = lax.map(one_angle, (amplitude, offsets, object_field))
    new_probe = probe_field + jnp.sum(numers, axis=0) / (jnp.sum(denoms, axis=0) + 1.0)
    sinogram = jnp.transpose(new_object[:, 1], (1, 0, 2))
    filtered = jnp.dot(sinogram.reshape(NOBJ * ANGLES, NOBJ), ramp_matrix(NOBJ), precision=lax.Precision.HIGHEST)
    filtered = jnp.moveaxis(filtered.reshape(NOBJ, ANGLES, NOBJ), 1, 0)

    def project_back(total, inputs):
        rows_angle, index_angle, weight_angle = inputs
        lower = jnp.take(rows_angle, index_angle, axis=1)
        upper = jnp.take(rows_angle, index_angle + 1, axis=1)
        return total + (1.0 - weight_angle) * lower + weight_angle * upper, None

    total, unused = lax.scan(project_back, jnp.zeros((NOBJ, ZWIN * NOBJ), jnp.float32),
                             (filtered, interp_index.reshape(ANGLES, ZWIN * NOBJ), interp_weight.reshape(ANGLES, ZWIN * NOBJ)))
    recon = (total * (math.pi / ANGLES)).reshape(N_POS, NOBJ // N_POS, ZWIN, NOBJ)
    return new_object, new_probe, recon
```

```python
import math

import numpy as np
import jax
import jax.numpy as jnp
from jax import lax
from jax.experimental import pallas as pl
from jax.experimental.pallas import tpu as pltpu
from jax.sharding import PartitionSpec as P

LANES = 128
ROWS = 8
BINS = 256


def passed_along(array, axis, by):
    length = lax.axis_size(axis)
    pairs = [(i, i + by) for i in range(length) if 0 <= i + by < length]
    return lax.ppermute(array, axis, pairs)


def split_halves(value):
    high = value.astype(jnp.bfloat16)
    low = (value - high.astype(jnp.float32)).astype(jnp.bfloat16)
    return high, low


def dft_tables(length):
    phases = np.outer(np.arange(length), np.arange(length)) % length
    theta = phases * (2.0 * math.pi / length)
    real = np.cos(theta) / math.sqrt(length)
    imag = -np.sin(theta) / math.sqrt(length)
    table = np.block([[real, imag], [-imag, real]]).astype(np.float32)
    tables = []
    for each in (table, table.T):
        high = each.astype(jnp.bfloat16)
        low = (each - high.astype(np.float32)).astype(jnp.bfloat16)
        tables += [high, low]
    return np.stack(tables)


def product(left, right):
    (left_high, left_low), (right_high, right_low) = left, right

    def dot(a, b):
        return jnp.dot(a, b, preferred_element_type=jnp.float32)

    return dot(left_high, right_high) + (dot(left_high, right_low) + dot(left_low, right_high))


def gradient_kernel(places, low_ref, block_ref, high_ref, probe_ref, amp_ref, table_ref,
                    up_ref, own_ref, down_ref, stat_ref, field, total):
    count, patch = amp_ref.shape[0], amp_ref.shape[1]
    half, band, width = low_ref.shape[1], block_ref.shape[1], block_ref.shape[2]
    field[:, :half] = low_ref[...]
    field[:, half:half + band] = block_ref[...]
    field[:, half + band:] = high_ref[...]
    total[...] = jnp.zeros(total.shape, jnp.float32)
    probe_real = probe_ref[0]
    probe_imag = probe_ref[1]
    power = probe_real * probe_real + probe_imag * probe_imag
    window = patch + LANES
    tall = patch + ROWS
    last = (width - window) // LANES
    spots = []
    patches = []
    waves = []
    for b in range(count):
        row = places[b, 0]
        col = places[b, 1]
        top = pl.multiple_of(row // ROWS * ROWS, ROWS)
        base = pl.multiple_of(jnp.minimum(col // LANES, last) * LANES, LANES)
        drop = row - top
        shift = col - base
        spots.append((top, drop, base, shift))
        cut = []
        for ch in range(2):
            wide = field[ch, pl.ds(top, tall), pl.ds(base, window)]
            narrow = pltpu.roll(wide, lax.rem(window - shift, window), 1)[:, :patch]
            cut.append(pltpu.roll(narrow, lax.rem(tall - drop, tall), 0)[:patch])
        patches.append(cut)
        waves.append((probe_real * cut[0] - probe_imag * cut[1], probe_real * cut[1] + probe_imag * cut[0]))
    forward = (table_ref[0], table_ref[1])
    backward = (table_ref[2], table_ref[3])

    def by_rows(pairs):
        return jnp.concatenate([jnp.concatenate(pair, axis=1) for pair in pairs], axis=0)

    def by_columns(pairs):
        return jnp.concatenate([jnp.concatenate(pair, axis=0) for pair in pairs], axis=1)

    def from_rows(whole):
        return [(whole[b * patch:(b + 1) * patch, :patch], whole[b * patch:(b + 1) * patch, patch:]) for b in range(count)]

    def from_columns(whole):
        return [(whole[:patch, b * patch:(b + 1) * patch], whole[patch:, b * patch:(b + 1) * patch]) for b in range(count)]

    middle = from_rows(product(split_halves(by_rows(waves)), forward))
    spectra = from_columns(product(backward, split_halves(by_columns(middle))))
    fixed = []
    for b in range(count):
        real, imag = spectra[b]
        factor = amp_ref[b] / jnp.maximum(jnp.sqrt(real * real + imag * imag), 0.5)
        fixed.append((factor * real, factor * imag))
    middle = from_columns(product(forward, split_halves(by_columns(fixed))))
    back = from_rows(product(split_halves(by_rows(middle)), backward))
    numer_real = jnp.zeros((patch, patch), jnp.float32)
    numer_imag = jnp.zeros((patch, patch), jnp.float32)
    denom = jnp.zeros((patch, patch), jnp.float32)
    blank = jnp.zeros((tall, LANES), jnp.float32)
    blank_rows = jnp.zeros((ROWS, patch), jnp.float32)
    for b in range(count):
        top, drop, base, shift = spots[b]
        cut_real, cut_imag = patches[b]
        diff_real = back[b][0] - waves[b][0]
        diff_imag = back[b][1] - waves[b][1]
        numer_real += cut_real * diff_real + cut_imag * diff_imag
        numer_imag += cut_real * diff_imag - cut_imag * diff_real
        denom += cut_real * cut_real + cut_imag * cut_imag
        terms = (probe_real * diff_real + probe_imag * diff_imag,
                 probe_real * diff_imag - probe_imag * diff_real, power)
        for ch, term in enumerate(terms):
            tall_term = pltpu.roll(jnp.concatenate([term, blank_rows], axis=0), drop, 0)
            wide = pltpu.roll(jnp.concatenate([tall_term, blank], axis=1), shift, 1)
            spot = (ch, pl.ds(top, tall), pl.ds(base, window))
            total[spot] = total[spot] + wide
    stat_ref[0] = numer_real
    stat_ref[1] = numer_imag
    stat_ref[2] = denom
    up_ref[...] = total[:, :half]
    own_ref[...] = total[:, half:half + band]
    down_ref[...] = total[:, half + band:]


def update_kernel(object_ref, own_ref, above_ref, below_ref, out_ref, imag_ref):
    band = own_ref.shape[1]
    half = above_ref.shape[1]
    ends = sorted({0, half, band - half, band})
    for start, stop in zip(ends[:-1], ends[1:]):
        terms = [own_ref[ch, start:stop] for ch in range(3)]
        if stop <= half:
            terms = [terms[ch] + above_ref[ch, start:stop] for ch in range(3)]
        if start >= band - half:
            offset = band - half
            terms = [terms[ch] + below_ref[ch, start - offset:stop - offset] for ch in range(3)]
        scale = terms[2] + 1.0
        out_ref[0, start:stop] = object_ref[0, start:stop] + terms[0] / scale
        imag = object_ref[1, start:stop] + terms[1] / scale
        out_ref[1, start:stop] = imag
        imag_ref[start:stop] = imag


def ramp_kernel(high_ref, low_ref):
    rows, width = high_ref.shape
    line = lax.broadcasted_iota(jnp.int32, (rows, width), 0) + pl.program_id(0) * rows
    differ = line - lax.broadcasted_iota(jnp.int32, (rows, width), 1)
    spread = differ.astype(jnp.float32)
    squared = jnp.maximum(spread * spread, 1.0)
    odd_terms = jnp.where((differ & 1) != 0, (-1.0 / (math.pi * math.pi)) / squared, 0.0)
    high, low = split_halves(jnp.where(differ == 0, 0.25, odd_terms))
    high_ref[...] = high
    low_ref[...] = low


def back_kernel(sino_ref, ramp_high_ref, ramp_low_ref, index_ref, weight_ref, out_ref, parts):
    angles, rows, width = sino_ref.shape
    depth = index_ref.shape[1]
    columns = index_ref.shape[2]

    @pl.when(pl.program_id(0) == 0)
    def _():
        sino = sino_ref[...].reshape(angles * rows, width)
        filtered = product(split_halves(sino), (ramp_high_ref[...], ramp_low_ref[...])) * (math.pi / angles)
        change = pltpu.roll(filtered, width - 1, 1) - filtered
        pieces = split_halves(filtered) + split_halves(change)
        for a in range(angles):
            for i in range(4):
                parts[a, i * rows:(i + 1) * rows] = pieces[i][a * rows:(a + 1) * rows]

    bins = lax.broadcasted_iota(jnp.int32, (width, columns), 0)
    for z in range(depth):
        result = jnp.zeros((rows, columns), jnp.float32)
        for a in range(angles):
            chosen = jnp.where(bins == index_ref[a, z:z + 1, :], 1.0, 0.0).astype(jnp.bfloat16)
            got = jnp.dot(parts[a], chosen, preferred_element_type=jnp.float32)
            lower = got[:rows] + got[rows:2 * rows]
            rise = got[2 * rows:3 * rows] + got[3 * rows:]
            result += lower + weight_ref[a, z:z + 1, :] * rise
        out_ref[:, z, :] = result


def on_device(amplitude, offsets, probe_field, object_field, interp_index, interp_weight):
    f32 = jnp.float32
    band = object_field.shape[2]
    width = object_field.shape[3]
    patch = probe_field.shape[1]
    half = patch // 2
    vmem = pl.BlockSpec(memory_space=pltpu.VMEM)
    smem = pl.BlockSpec(memory_space=pltpu.SMEM)
    layer = object_field[0]
    low = passed_along(layer[:, band - half:], "pos", 1)
    high = passed_along(layer[:, :half], "pos", -1)
    anchor = lax.axis_index("pos") * band - half
    places = offsets[0] - jnp.stack([anchor, 0]).astype(jnp.int32)
    up, own, down, stats = pl.pallas_call(
        gradient_kernel,
        name="gradient",
        out_shape=(
            jax.ShapeDtypeStruct((3, half, width), f32),
            jax.ShapeDtypeStruct((3, band, width), f32),
            jax.ShapeDtypeStruct((3, half, width), f32),
            jax.ShapeDtypeStruct((3, patch, patch), f32),
        ),
        in_specs=[smem] + [vmem] * 6,
        out_specs=[vmem] * 4,
        scratch_shapes=[pltpu.VMEM((2, band + patch, width), f32), pltpu.VMEM((3, band + patch, width), f32)],
    )(places, low, layer, high, probe_field, amplitude[0], dft_tables(patch))
    from_below = passed_along(up, "pos", -1)
    from_above = passed_along(down, "pos", 1)
    ramp_rows = width // 4
    ramp_high, ramp_low = pl.pallas_call(
        ramp_kernel,
        name="ramp",
        grid=(width // ramp_rows,),
        out_shape=(jax.ShapeDtypeStruct((width, width), jnp.bfloat16),) * 2,
        out_specs=[pl.BlockSpec((ramp_rows, width), lambda i: (i, 0))] * 2,
        cost_estimate=pl.CostEstimate(flops=20 * width * width, transcendentals=0, bytes_accessed=4 * width * width),
    )()
    new_layer, imag = pl.pallas_call(
        update_kernel,
        name="update",
        out_shape=(jax.ShapeDtypeStruct((2, band, width), f32), jax.ShapeDtypeStruct((band, width), f32)),
        in_specs=[vmem] * 4,
        out_specs=[vmem] * 2,
    )(layer, own, from_above, from_below)
    everyone = ("angle", "pos")
    shares = lax.axis_size("angle") * lax.axis_size("pos")
    angles = lax.axis_size("angle")
    regrouped = lax.all_to_all(imag.reshape(angles, band // angles, width), "angle", split_axis=0, concat_axis=0, tiled=True)
    pieces = jnp.swapaxes(stats.reshape(3, shares, -1), 0, 1)
    mine = jnp.sum(lax.all_to_all(pieces, everyone, split_axis=0, concat_axis=0, tiled=True), axis=0)
    step = mine[:2] / (mine[2:] + 1.0)
    steps = lax.all_gather(step, everyone, axis=0, tiled=False)
    new_probe = probe_field + jnp.swapaxes(steps, 0, 1).reshape(probe_field.shape)
    rows = band // angles
    zwin = interp_index.shape[1]
    columns = min(BINS, width)
    recon = pl.pallas_call(
        back_kernel,
        name="back",
        grid=(width // columns,),
        out_shape=jax.ShapeDtypeStruct((rows, zwin, width), f32),
        in_specs=[
            pl.BlockSpec((angles, rows, width), lambda i: (0, 0, 0)),
            pl.BlockSpec((width, width), lambda i: (0, 0)),
            pl.BlockSpec((width, width), lambda i: (0, 0)),
            pl.BlockSpec((angles, zwin, columns), lambda i: (0, 0, i)),
            pl.BlockSpec((angles, zwin, columns), lambda i: (0, 0, i)),
        ],
        out_specs=pl.BlockSpec((rows, zwin, columns), lambda i: (0, 0, i)),
        scratch_shapes=[pltpu.VMEM((angles, 4 * rows, width), jnp.bfloat16)],
        compiler_params=pltpu.CompilerParams(dimension_semantics=("arbitrary",)),
    )(regrouped, ramp_high, ramp_low, interp_index, interp_weight)
    return (new_layer[None], new_probe, recon[None])


def solution(mesh):
    placed = (
        P("angle", "pos", None, None),
        P("angle", "pos", None),
        P(),
        P("angle", None, "pos", None),
        P(),
        P(),
    )
    return jax.shard_map(
        on_device,
        mesh=mesh,
        in_specs=placed,
        out_specs=(P("angle", None, "pos", None), P(), P("pos", "angle", None, None)),
        check_vma=False,
    )
```

```python
import math

import numpy as np
import jax
import jax.numpy as jnp
from jax import lax
from jax.experimental import pallas as pl
from jax.experimental.pallas import tpu as pltpu
from jax.sharding import PartitionSpec as P

LANES = 128
ROWS = 8
BINS = 256


def passed_along(array, axis, by):
    length = lax.axis_size(axis)
    pairs = [(i, i + by) for i in range(length) if 0 <= i + by < length]
    return lax.ppermute(array, axis, pairs)


def split_halves(value):
    high = value.astype(jnp.bfloat16)
    low = (value - high.astype(jnp.float32)).astype(jnp.bfloat16)
    return high, low


def dft_tables(length):
    phases = np.outer(np.arange(length), np.arange(length)) % length
    theta = phases * (2.0 * math.pi / length)
    real = np.cos(theta) / math.sqrt(length)
    imag = -np.sin(theta) / math.sqrt(length)
    table = np.block([[real, imag], [-imag, real]]).astype(np.float32)
    tables = []
    for each in (table, table.T):
        high = each.astype(jnp.bfloat16)
        low = (each - high.astype(np.float32)).astype(jnp.bfloat16)
        tables += [high, low]
    return np.stack(tables)


def product(left, right):
    (left_high, left_low), (right_high, right_low) = left, right

    def dot(a, b):
        return jnp.dot(a, b, preferred_element_type=jnp.float32)

    return dot(left_high, right_high) + (dot(left_high, right_low) + dot(left_low, right_high))


def gradient_kernel(places, low_ref, block_ref, high_ref, probe_ref, amp_ref, table_ref, ramp_ref,
                    up_ref, own_ref, down_ref, stat_ref, field, total):
    count, patch = amp_ref.shape[0], amp_ref.shape[1]
    half, band, width = low_ref.shape[1], block_ref.shape[1], block_ref.shape[2]
    field[:, :half] = low_ref[...]
    field[:, half:half + band] = block_ref[...]
    field[:, half + band:] = high_ref[...]
    total[...] = jnp.zeros(total.shape, jnp.float32)
    probe_real = probe_ref[0]
    probe_imag = probe_ref[1]
    power = probe_real * probe_real + probe_imag * probe_imag
    window = patch + LANES
    tall = patch + ROWS
    last = (width - window) // LANES
    spots = []
    patches = []
    waves = []
    for b in range(count):
        row = places[b, 0]
        col = places[b, 1]
        top = pl.multiple_of(row // ROWS * ROWS, ROWS)
        base = pl.multiple_of(jnp.minimum(col // LANES, last) * LANES, LANES)
        drop = row - top
        shift = col - base
        spots.append((top, drop, base, shift))
        cut = []
        for ch in range(2):
            wide = field[ch, pl.ds(top, tall), pl.ds(base, window)]
            narrow = pltpu.roll(wide, lax.rem(window - shift, window), 1)[:, :patch]
            cut.append(pltpu.roll(narrow, lax.rem(tall - drop, tall), 0)[:patch])
        patches.append(cut)
        waves.append((probe_real * cut[0] - probe_imag * cut[1], probe_real * cut[1] + probe_imag * cut[0]))
    forward = (table_ref[0], table_ref[1])
    backward = (table_ref[2], table_ref[3])

    def by_rows(pairs):
        return jnp.concatenate([jnp.concatenate(pair, axis=1) for pair in pairs], axis=0)

    def by_columns(pairs):
        return jnp.concatenate([jnp.concatenate(pair, axis=0) for pair in pairs], axis=1)

    def from_rows(whole):
        return [(whole[b * patch:(b + 1) * patch, :patch], whole[b * patch:(b + 1) * patch, patch:]) for b in range(count)]

    def from_columns(whole):
        return [(whole[:patch, b * patch:(b + 1) * patch], whole[patch:, b * patch:(b + 1) * patch]) for b in range(count)]

    middle = from_rows(product(split_halves(by_rows(waves)), forward))
    spectra = from_columns(product(backward, split_halves(by_columns(middle))))
    fixed = []
    for b in range(count):
        real, imag = spectra[b]
        factor = amp_ref[b] / jnp.maximum(jnp.sqrt(real * real + imag * imag), 0.5)
        fixed.append((factor * real, factor * imag))
    middle = from_columns(product(forward, split_halves(by_columns(fixed))))
    back = from_rows(product(split_halves(by_rows(middle)), backward))
    numer_real = jnp.zeros((patch, patch), jnp.float32)
    numer_imag = jnp.zeros((patch, patch), jnp.float32)
    denom = jnp.zeros((patch, patch), jnp.float32)
    blank = jnp.zeros((tall, LANES), jnp.float32)
    blank_rows = jnp.zeros((ROWS, patch), jnp.float32)
    for b in range(count):
        top, drop, base, shift = spots[b]
        cut_real, cut_imag = patches[b]
        diff_real = back[b][0] - waves[b][0]
        diff_imag = back[b][1] - waves[b][1]
        numer_real += cut_real * diff_real + cut_imag * diff_imag
        numer_imag += cut_real * diff_imag - cut_imag * diff_real
        denom += cut_real * cut_real + cut_imag * cut_imag
        terms = (probe_real * diff_real + probe_imag * diff_imag,
                 probe_real * diff_imag - probe_imag * diff_real, power)
        for ch, term in enumerate(terms):
            tall_term = pltpu.roll(jnp.concatenate([term, blank_rows], axis=0), drop, 0)
            wide = pltpu.roll(jnp.concatenate([tall_term, blank], axis=1), shift, 1)
            spot = (ch, pl.ds(top, tall), pl.ds(base, window))
            total[spot] = total[spot] + wide
    stat_ref[:, 0, :] = numer_real
    stat_ref[:, 1, :] = numer_imag
    stat_ref[:, 2, :] = denom
    up_ref[...] = total[:, :half]
    own_ref[...] = total[:, half:half + band]
    down_ref[...] = total[:, half + band:]


def update_kernel(object_ref, own_ref, above_ref, below_ref, out_ref, imag_ref):
    band = own_ref.shape[1]
    half = above_ref.shape[1]
    ends = sorted({0, half, band - half, band})
    for start, stop in zip(ends[:-1], ends[1:]):
        terms = [own_ref[ch, start:stop] for ch in range(3)]
        if stop <= half:
            terms = [terms[ch] + above_ref[ch, start:stop] for ch in range(3)]
        if start >= band - half:
            offset = band - half
            terms = [terms[ch] + below_ref[ch, start - offset:stop - offset] for ch in range(3)]
        scale = terms[2] + 1.0
        out_ref[0, start:stop] = object_ref[0, start:stop] + terms[0] / scale
        imag = object_ref[1, start:stop] + terms[1] / scale
        out_ref[1, start:stop] = imag
        imag_ref[start:stop] = imag


def ramp_kernel(high_ref, low_ref):
    rows, width = high_ref.shape
    line = lax.broadcasted_iota(jnp.int32, (rows, width), 0) + pl.program_id(0) * rows
    differ = line - lax.broadcasted_iota(jnp.int32, (rows, width), 1)
    spread = differ.astype(jnp.float32)
    squared = jnp.maximum(spread * spread, 1.0)
    odd_terms = jnp.where((differ & 1) != 0, (-1.0 / (math.pi * math.pi)) / squared, 0.0)
    high, low = split_halves(jnp.where(differ == 0, 0.25, odd_terms))
    high_ref[...] = high
    low_ref[...] = low


def back_kernel(sino_ref, ramp_high_ref, ramp_low_ref, index_ref, weight_ref, out_ref, parts):
    angles, rows, width = sino_ref.shape
    depth = index_ref.shape[1]
    columns = index_ref.shape[2]

    @pl.when(pl.program_id(0) == 0)
    def _():
        sino = sino_ref[...].reshape(angles * rows, width)
        filtered = product(split_halves(sino), (ramp_high_ref[...], ramp_low_ref[...])) * (math.pi / angles)
        change = pltpu.roll(filtered, width - 1, 1) - filtered
        pieces = split_halves(filtered) + split_halves(change)
        for a in range(angles):
            for i in range(4):
                parts[a, i * rows:(i + 1) * rows] = pieces[i][a * rows:(a + 1) * rows]

    bins = lax.broadcasted_iota(jnp.int32, (width, columns), 0)
    for z in range(depth):
        result = jnp.zeros((rows, columns), jnp.float32)
        for a in range(angles):
            chosen = jnp.where(bins == index_ref[a, z:z + 1, :], 1.0, 0.0).astype(jnp.bfloat16)
            got = jnp.dot(parts[a], chosen, preferred_element_type=jnp.float32)
            lower = got[:rows] + got[rows:2 * rows]
            rise = got[2 * rows:3 * rows] + got[3 * rows:]
            result += lower + weight_ref[a, z:z + 1, :] * rise
        out_ref[:, z, :] = result


def on_device(amplitude, offsets, probe_field, object_field, interp_index, interp_weight):
    f32 = jnp.float32
    band = object_field.shape[2]
    width = object_field.shape[3]
    patch = probe_field.shape[1]
    half = patch // 2
    vmem = pl.BlockSpec(memory_space=pltpu.VMEM)
    smem = pl.BlockSpec(memory_space=pltpu.SMEM)
    layer = object_field[0]
    low = passed_along(layer[:, band - half:], "pos", 1)
    high = passed_along(layer[:, :half], "pos", -1)
    anchor = lax.axis_index("pos") * band - half
    places = offsets[0] - jnp.stack([anchor, 0]).astype(jnp.int32)
    ramp_rows = width // 4
    ramp_high, ramp_low = pl.pallas_call(
        ramp_kernel,
        name="ramp",
        grid=(width // ramp_rows,),
        out_shape=(jax.ShapeDtypeStruct((width, width), jnp.bfloat16),) * 2,
        out_specs=[pl.BlockSpec((ramp_rows, width), lambda i: (i, 0))] * 2,
        cost_estimate=pl.CostEstimate(flops=20 * width * width, transcendentals=0, bytes_accessed=4 * width * width),
    )()
    up, own, down, stats = pl.pallas_call(
        gradient_kernel,
        name="gradient",
        out_shape=(
            jax.ShapeDtypeStruct((3, half, width), f32),
            jax.ShapeDtypeStruct((3, band, width), f32),
            jax.ShapeDtypeStruct((3, half, width), f32),
            jax.ShapeDtypeStruct((patch, 3, patch), f32),
        ),
        in_specs=[smem] + [vmem] * 6 + [pl.BlockSpec(memory_space=pl.ANY)],
        out_specs=[vmem] * 4,
        scratch_shapes=[pltpu.VMEM((2, band + patch, width), f32), pltpu.VMEM((3, band + patch, width), f32)],
    )(places, low, layer, high, probe_field, amplitude[0], dft_tables(patch), ramp_high)
    from_below = passed_along(up, "pos", -1)
    from_above = passed_along(down, "pos", 1)
    new_layer, imag = pl.pallas_call(
        update_kernel,
        name="update",
        out_shape=(jax.ShapeDtypeStruct((2, band, width), f32), jax.ShapeDtypeStruct((band, width), f32)),
        in_specs=[vmem] * 4,
        out_specs=[vmem] * 2,
    )(layer, own, from_above, from_below)
    everyone = ("angle", "pos")
    shares = lax.axis_size("angle") * lax.axis_size("pos")
    angles = lax.axis_size("angle")
    regrouped = lax.all_to_all(imag.reshape(angles, band // angles, width), "angle", split_axis=0, concat_axis=0, tiled=True)
    pieces = stats.reshape(shares, patch // shares, 3, patch)
    mine = jnp.sum(lax.all_to_all(pieces, everyone, split_axis=0, concat_axis=0, tiled=True), axis=0)
    step = mine[:, :2] / (mine[:, 2:] + 1.0)
    copies = jnp.broadcast_to(step[None], (shares,) + step.shape)
    steps = lax.all_to_all(copies, everyone, split_axis=0, concat_axis=0, tiled=True)
    new_probe = probe_field + jnp.swapaxes(steps.reshape(patch, 2, patch), 0, 1)
    rows = band // angles
    zwin = interp_index.shape[1]
    columns = min(BINS, width)
    recon = pl.pallas_call(
        back_kernel,
        name="back",
        grid=(width // columns,),
        out_shape=jax.ShapeDtypeStruct((rows, zwin, width), f32),
        in_specs=[
            pl.BlockSpec((angles, rows, width), lambda i: (0, 0, 0)),
            pl.BlockSpec((width, width), lambda i: (0, 0)),
            pl.BlockSpec((width, width), lambda i: (0, 0)),
            pl.BlockSpec((angles, zwin, columns), lambda i: (0, 0, i)),
            pl.BlockSpec((angles, zwin, columns), lambda i: (0, 0, i)),
        ],
        out_specs=pl.BlockSpec((rows, zwin, columns), lambda i: (0, 0, i)),
        scratch_shapes=[pltpu.VMEM((angles, 4 * rows, width), jnp.bfloat16)],
        compiler_params=pltpu.CompilerParams(dimension_semantics=("arbitrary",)),
    )(regrouped, ramp_high, ramp_low, interp_index, interp_weight)
    return (new_layer[None], new_probe, recon[None])


def solution(mesh):
    placed = (
        P("angle", "pos", None, None),
        P("angle", "pos", None),
        P(),
        P("angle", None, "pos", None),
        P(),
        P(),
    )
    return jax.shard_map(
        on_device,
        mesh=mesh,
        in_specs=placed,
        out_specs=(P("angle", None, "pos", None), P(), P("pos", "angle", None, None)),
        check_vma=False,
    )
```

```python
import math

import numpy as np
import jax
import jax.numpy as jnp
from jax import lax
from jax.experimental import pallas as pl
from jax.experimental.pallas import tpu as pltpu
from jax.sharding import PartitionSpec as P


LANES = 128
ROWS = 8
BINS = 256


def passed_along(array, axis, by):
    length = lax.axis_size(axis)
    pairs = [(i, i + by) for i in range(length) if 0 <= i + by < length]
    return lax.ppermute(array, axis, pairs)


def split_halves(value):
    high = value.astype(jnp.bfloat16)
    low = (value - high.astype(jnp.float32)).astype(jnp.bfloat16)
    return high, low


def dft_tables(length):
    phases = np.outer(np.arange(length), np.arange(length)) % length
    theta = phases * (2.0 * math.pi / length)
    real = np.cos(theta) / math.sqrt(length)
    imag = -np.sin(theta) / math.sqrt(length)
    table = np.block([[real, imag], [-imag, real]]).astype(np.float32)
    tables = []
    for each in (table, table.T):
        high = each.astype(jnp.bfloat16)
        low = (each - high.astype(np.float32)).astype(jnp.bfloat16)
        tables += [high, low]
    return np.stack(tables)


def product(left, right):
    (left_high, left_low), (right_high, right_low) = left, right

    def dot(a, b):
        return jnp.dot(a, b, preferred_element_type=jnp.float32)

    return dot(left_high, right_high) + (dot(left_high, right_low) + dot(left_low, right_high))


def row_spot(row):
    top = pl.multiple_of(row // ROWS * ROWS, ROWS)
    return top, row - top


def column_spot(col, last):
    base = pl.multiple_of(jnp.minimum(col // LANES, last) * LANES, LANES)
    return base, col - base


def spread_rows(column, term, top, drop):
    tall = term.shape[0] + ROWS
    column[...] = jnp.zeros(column.shape, jnp.float32)
    blank = jnp.zeros((ROWS, term.shape[1]), jnp.float32)
    column[pl.ds(top, tall)] = pltpu.roll(jnp.concatenate([term, blank], axis=0), drop, 0)


def add_columns(ref, lead, term, base, shift):
    blank = jnp.zeros((term.shape[0], LANES), jnp.float32)
    wide = pltpu.roll(jnp.concatenate([term, blank], axis=1), shift, 1)
    spot = lead + (pl.ds(base, term.shape[1] + LANES),)
    ref[spot] = ref[spot] + wide


def pack_kernel(places, block_ref, up_ref, down_ref):
    band, width = block_ref.shape[1], block_ref.shape[2]
    half = (up_ref.shape[0] - ROWS) // 2
    lane = lax.broadcasted_iota(jnp.int32, (ROWS, width), 1)
    note = jnp.zeros((ROWS, width), jnp.int32)
    for b in range(places.shape[0]):
        for i in range(2):
            note = jnp.where(lane == 2 * b + i, places[b, i] + 1, note)
    note = note.astype(jnp.float32)
    for ch in range(2):
        up_ref[ch * half:(ch + 1) * half] = block_ref[ch, :half]
        down_ref[ch * half:(ch + 1) * half] = block_ref[ch, band - half:]
    up_ref[2 * half:] = note
    down_ref[2 * half:] = note


def weight_kernel(near, probe_ref, out_ref, total, column):
    band, width = out_ref.shape
    patch = probe_ref.shape[1]
    half = patch // 2
    last = width // LANES - patch // LANES - 1
    power = probe_ref[0] * probe_ref[0] + probe_ref[1] * probe_ref[1]
    total[...] = jnp.ones(total.shape, jnp.float32)
    for b in range(near.shape[0]):
        group = b * 3 // near.shape[0]
        top, drop = row_spot(near[b, 0])
        base, shift = column_spot(near[b, 1], last)
        term = power * near[b, 2].astype(jnp.float32)
        slot = column.at[b % 2]
        spread_rows(slot, term, top, drop)
        if group == 0:
            add_columns(total, (slice(None),), slot[half:half + band], base, shift)
        elif group == 1:
            add_columns(total, (slice(0, half),), slot[half + band:], base, shift)
        else:
            add_columns(total, (slice(band - half, band),), slot[:half], base, shift)
    out_ref[...] = 1.0 / total[...]


def gradient_kernel(places, low_ref, block_ref, high_ref, probe_ref, amp_ref, table_ref, ramp_ref,
                    up_ref, own_ref, down_ref, stat_ref, field, column):
    count, patch = amp_ref.shape[0], amp_ref.shape[1]
    half, band, width = patch // 2, block_ref.shape[1], block_ref.shape[2]
    field[:, half:half + band] = block_ref[...]
    for ch in range(2):
        field[ch, :half] = low_ref[ch * half:(ch + 1) * half]
        field[ch, half + band:] = high_ref[ch * half:(ch + 1) * half]
    own_ref[...] = jnp.zeros(own_ref.shape, jnp.float32)
    probe_real = probe_ref[0]
    probe_imag = probe_ref[1]
    window = patch + LANES
    tall = patch + ROWS
    last = (width - window) // LANES
    spots = []
    patches = []
    waves = []
    for b in range(count):
        row = places[b, 0]
        col = places[b, 1]
        top, drop = row_spot(row)
        base, shift = column_spot(col, last)
        spots.append((top, drop, base, shift))
        cut = []
        for ch in range(2):
            wide = field[ch, pl.ds(top, tall), pl.ds(base, window)]
            narrow = pltpu.roll(wide, lax.rem(window - shift, window), 1)[:, :patch]
            cut.append(pltpu.roll(narrow, lax.rem(tall - drop, tall), 0)[:patch])
        patches.append(cut)
        waves.append((probe_real * cut[0] - probe_imag * cut[1], probe_real * cut[1] + probe_imag * cut[0]))
    forward = (table_ref[0], table_ref[1])
    backward = (table_ref[2], table_ref[3])

    def by_rows(pairs):
        return jnp.concatenate([jnp.concatenate(pair, axis=1) for pair in pairs], axis=0)

    def by_columns(pairs):
        return jnp.concatenate([jnp.concatenate(pair, axis=0) for pair in pairs], axis=1)

    def from_rows(whole):
        return [(whole[b * patch:(b + 1) * patch, :patch], whole[b * patch:(b + 1) * patch, patch:]) for b in range(count)]

    def from_columns(whole):
        return [(whole[:patch, b * patch:(b + 1) * patch], whole[patch:, b * patch:(b + 1) * patch]) for b in range(count)]

    middle = from_rows(product(split_halves(by_rows(waves)), forward))
    spectra = from_columns(product(backward, split_halves(by_columns(middle))))
    fixed = []
    for b in range(count):
        real, imag = spectra[b]
        factor = amp_ref[b] / jnp.maximum(jnp.sqrt(real * real + imag * imag), 0.5)
        fixed.append((factor * real, factor * imag))
    middle = from_columns(product(forward, split_halves(by_columns(fixed))))
    back = from_rows(product(split_halves(by_rows(middle)), backward))
    numer_real = jnp.zeros((patch, patch), jnp.float32)
    numer_imag = jnp.zeros((patch, patch), jnp.float32)
    denom = jnp.zeros((patch, patch), jnp.float32)
    for b in range(count):
        top, drop, base, shift = spots[b]
        cut_real, cut_imag = patches[b]
        diff_real = back[b][0] - waves[b][0]
        diff_imag = back[b][1] - waves[b][1]
        numer_real += cut_real * diff_real + cut_imag * diff_imag
        numer_imag += cut_real * diff_imag - cut_imag * diff_real
        denom += cut_real * cut_real + cut_imag * cut_imag
        terms = (probe_real * diff_real + probe_imag * diff_imag,
                 probe_real * diff_imag - probe_imag * diff_real)
        for ch, term in enumerate(terms):
            spread_rows(column.at[ch], term, top, drop)
            up_ref[ch, b] = column[ch, :half]
            add_columns(own_ref, (ch, slice(None)), column[ch, half:half + band], base, shift)
            down_ref[ch, b] = column[ch, half + band:]
    stat_ref[:, 0, :] = numer_real
    stat_ref[:, 1, :] = numer_imag
    stat_ref[:, 2, :] = denom


def update_kernel(near, object_ref, own_ref, weight_ref, above_ref, below_ref, out_ref, imag_ref, total):
    band, width = own_ref.shape[1], own_ref.shape[2]
    count, half, patch = above_ref.shape[1], above_ref.shape[2], above_ref.shape[3]
    last = width // LANES - patch // LANES - 1
    total[...] = own_ref[...]
    for b in range(count):
        for group, ref, start in ((1, above_ref, 0), (2, below_ref, band - half)):
            base, shift = column_spot(near[group * count + b, 1], last)
            for ch in range(2):
                add_columns(total, (ch, slice(start, start + half)), ref[ch, b], base, shift)
    scale = weight_ref[...]
    out_ref[0] = object_ref[0] + total[0] * scale
    imag = object_ref[1] + total[1] * scale
    out_ref[1] = imag
    imag_ref[...] = imag


def ramp_kernel(high_ref, low_ref):
    rows, width = high_ref.shape
    line = lax.broadcasted_iota(jnp.int32, (rows, width), 0) + pl.program_id(0) * rows
    differ = line - lax.broadcasted_iota(jnp.int32, (rows, width), 1)
    spread = differ.astype(jnp.float32)
    squared = jnp.maximum(spread * spread, 1.0)
    odd_terms = jnp.where((differ & 1) != 0, (-1.0 / (math.pi * math.pi)) / squared, 0.0)
    high, low = split_halves(jnp.where(differ == 0, 0.25, odd_terms))
    high_ref[...] = high
    low_ref[...] = low


def back_kernel(sino_ref, ramp_high_ref, ramp_low_ref, index_ref, weight_ref, out_ref, parts):
    angles, rows, width = sino_ref.shape
    depth = index_ref.shape[1]
    columns = index_ref.shape[2]

    @pl.when(pl.program_id(0) == 0)
    def _():
        sino = sino_ref[...].reshape(angles * rows, width)
        filtered = product(split_halves(sino), (ramp_high_ref[...], ramp_low_ref[...])) * (math.pi / angles)
        change = pltpu.roll(filtered, width - 1, 1) - filtered
        pieces = split_halves(filtered) + split_halves(change)
        for a in range(angles):
            for i in range(4):
                parts[a, i * rows:(i + 1) * rows] = pieces[i][a * rows:(a + 1) * rows]

    bins = lax.broadcasted_iota(jnp.int32, (width, columns), 0)
    for z in range(depth):
        result = jnp.zeros((rows, columns), jnp.float32)
        for a in range(angles):
            chosen = jnp.where(bins == index_ref[a, z:z + 1, :], 1.0, 0.0).astype(jnp.bfloat16)
            got = jnp.dot(parts[a], chosen, preferred_element_type=jnp.float32)
            lower = got[:rows] + got[rows:2 * rows]
            rise = got[2 * rows:3 * rows] + got[3 * rows:]
            result += lower + weight_ref[a, z:z + 1, :] * rise
        out_ref[:, z, :] = result


def on_device(amplitude, offsets, probe_field, object_field, interp_index, interp_weight):
    f32 = jnp.float32
    band = object_field.shape[2]
    width = object_field.shape[3]
    patch = probe_field.shape[1]
    half = patch // 2
    vmem = pl.BlockSpec(memory_space=pltpu.VMEM)
    smem = pl.BlockSpec(memory_space=pltpu.SMEM)
    layer = object_field[0]
    count = offsets.shape[1]
    packed = jax.ShapeDtypeStruct((2 * half + ROWS, width), f32)
    to_above, to_below = pl.pallas_call(
        pack_kernel,
        name="pack",
        out_shape=(packed, packed),
        in_specs=[smem, vmem],
        out_specs=[vmem] * 2,
    )(offsets[0], layer)
    low = passed_along(to_below, "pos", 1)
    high = passed_along(to_above, "pos", -1)
    anchor = lax.axis_index("pos") * band - half
    places = offsets[0] - jnp.stack([anchor, 0]).astype(jnp.int32)
    near = [jnp.concatenate([places, jnp.ones((count, 1), jnp.int32)], axis=1)]
    for message, far in ((low, anchor - band), (high, anchor + band)):
        note = message[2 * half, :2 * count].reshape(count, 2).astype(jnp.int32)
        valid = note[:, 1:] > 0
        there = note - 1 - jnp.stack([far, 0]).astype(jnp.int32)
        near.append(jnp.concatenate([jnp.where(valid, there, 0), valid.astype(jnp.int32)], axis=1))
    near = jnp.concatenate(near, axis=0)
    ramp_rows = width // 4
    ramp_high, ramp_low = pl.pallas_call(
        ramp_kernel,
        name="ramp",
        grid=(width // ramp_rows,),
        out_shape=(jax.ShapeDtypeStruct((width, width), jnp.bfloat16),) * 2,
        out_specs=[pl.BlockSpec((ramp_rows, width), lambda i: (i, 0))] * 2,
        cost_estimate=pl.CostEstimate(flops=20 * width * width, transcendentals=0, bytes_accessed=4 * width * width),
    )()
    up, own, down, stats = pl.pallas_call(
        gradient_kernel,
        name="gradient",
        out_shape=(
            jax.ShapeDtypeStruct((2, count, half, patch), f32),
            jax.ShapeDtypeStruct((2, band, width), f32),
            jax.ShapeDtypeStruct((2, count, half, patch), f32),
            jax.ShapeDtypeStruct((patch, 3, patch), f32),
        ),
        in_specs=[smem] + [vmem] * 6 + [pl.BlockSpec(memory_space=pl.ANY)],
        out_specs=[vmem] * 4,
        scratch_shapes=[pltpu.VMEM((2, band + patch, width), f32), pltpu.VMEM((2, band + patch, patch), f32)],
    )(places, low, layer, high, probe_field, amplitude[0], dft_tables(patch), ramp_high)
    from_below = passed_along(up, "pos", -1)
    from_above = passed_along(down, "pos", 1)
    weight = pl.pallas_call(
        weight_kernel,
        name="weight",
        out_shape=jax.ShapeDtypeStruct((band, width), f32),
        in_specs=[smem, vmem],
        out_specs=vmem,
        scratch_shapes=[pltpu.VMEM((band, width), f32), pltpu.VMEM((2, band + patch, patch), f32)],
        cost_estimate=pl.CostEstimate(flops=20 * width * width, transcendentals=0, bytes_accessed=4 * band * width),
    )(near, probe_field)
    new_layer, imag = pl.pallas_call(
        update_kernel,
        name="update",
        out_shape=(jax.ShapeDtypeStruct((2, band, width), f32), jax.ShapeDtypeStruct((band, width), f32)),
        in_specs=[smem] + [vmem] * 5,
        out_specs=[vmem] * 2,
        scratch_shapes=[pltpu.VMEM((2, band, width), f32)],
    )(near, layer, own, weight, from_above, from_below)
    everyone = ("angle", "pos")
    shares = lax.axis_size("angle") * lax.axis_size("pos")
    angles = lax.axis_size("angle")
    regrouped = lax.all_to_all(imag.reshape(angles, band // angles, width), "angle", split_axis=0, concat_axis=0, tiled=True)
    pieces = stats.reshape(shares, patch // shares, 3, patch)
    shared = lax.all_to_all(pieces, everyone, split_axis=0, concat_axis=0, tiled=True)
    mine = jnp.sum(shared, axis=0)
    step = mine[:, :2] / (mine[:, 2:] + 1.0)
    copies = jnp.broadcast_to(step[None], (shares,) + step.shape)
    copies, regrouped = lax.optimization_barrier((copies, regrouped))
    steps = lax.all_to_all(copies, everyone, split_axis=0, concat_axis=0, tiled=True)
    new_probe = probe_field + jnp.swapaxes(steps.reshape(patch, 2, patch), 0, 1)
    rows = band // angles
    zwin = interp_index.shape[1]
    columns = min(BINS, width)
    recon = pl.pallas_call(
        back_kernel,
        name="back",
        grid=(width // columns,),
        out_shape=jax.ShapeDtypeStruct((rows, zwin, width), f32),
        in_specs=[
            pl.BlockSpec((angles, rows, width), lambda i: (0, 0, 0)),
            pl.BlockSpec((width, width), lambda i: (0, 0)),
            pl.BlockSpec((width, width), lambda i: (0, 0)),
            pl.BlockSpec((angles, zwin, columns), lambda i: (0, 0, i)),
            pl.BlockSpec((angles, zwin, columns), lambda i: (0, 0, i)),
        ],
        out_specs=pl.BlockSpec((rows, zwin, columns), lambda i: (0, 0, i)),
        scratch_shapes=[pltpu.VMEM((angles, 4 * rows, width), jnp.bfloat16)],
        compiler_params=pltpu.CompilerParams(dimension_semantics=("arbitrary",)),
    )(regrouped, ramp_high, ramp_low, interp_index, interp_weight)
    return (new_layer[None], new_probe, recon[None])


def solution(mesh):
    placed = (
        P("angle", "pos", None, None),
        P("angle", "pos", None),
        P(),
        P("angle", None, "pos", None),
        P(),
        P(),
    )

    return jax.shard_map(
        on_device,
        mesh=mesh,
        in_specs=placed,
        out_specs=(P("angle", None, "pos", None), P(), P("pos", "angle", None, None)),
        check_vma=False,
    )
```

```python
import math

import numpy as np
import jax
import jax.numpy as jnp
from jax import lax
from jax.experimental import pallas as pl
from jax.experimental.pallas import tpu as pltpu
from jax.sharding import PartitionSpec as P


LANES = 128
ROWS = 8
BINS = 256


def passed_along(array, axis, by):
    length = lax.axis_size(axis)
    pairs = [(i, i + by) for i in range(length) if 0 <= i + by < length]
    return lax.ppermute(array, axis, pairs)


def split_halves(value):
    high = value.astype(jnp.bfloat16)
    low = (value - high.astype(jnp.float32)).astype(jnp.bfloat16)
    return high, low


def dft_tables(length):
    phases = np.outer(np.arange(length), np.arange(length)) % length
    theta = phases * (2.0 * math.pi / length)
    real = np.cos(theta) / math.sqrt(length)
    imag = -np.sin(theta) / math.sqrt(length)
    table = np.block([[real, imag], [-imag, real]]).astype(np.float32)
    tables = []
    for each in (table, table.T):
        high = each.astype(jnp.bfloat16)
        low = (each - high.astype(np.float32)).astype(jnp.bfloat16)
        tables += [high, low]
    return np.stack(tables)


def product(left, right):
    (left_high, left_low), (right_high, right_low) = left, right

    def dot(a, b):
        return jnp.dot(a, b, preferred_element_type=jnp.float32)

    return dot(left_high, right_high) + (dot(left_high, right_low) + dot(left_low, right_high))


def row_spot(row):
    top = pl.multiple_of(row // ROWS * ROWS, ROWS)
    return top, row - top


def column_spot(col, last):
    base = pl.multiple_of(jnp.minimum(col // LANES, last) * LANES, LANES)
    return base, col - base


def spread_rows(column, term, top, drop):
    tall = term.shape[0] + ROWS
    column[...] = jnp.zeros(column.shape, jnp.float32)
    blank = jnp.zeros((ROWS, term.shape[1]), jnp.float32)
    column[pl.ds(top, tall)] = pltpu.roll(jnp.concatenate([term, blank], axis=0), drop, 0)


def add_columns(ref, lead, term, base, shift):
    blank = jnp.zeros((term.shape[0], LANES), jnp.float32)
    wide = pltpu.roll(jnp.concatenate([term, blank], axis=1), shift, 1)
    spot = lead + (pl.ds(base, term.shape[1] + LANES),)
    ref[spot] = ref[spot] + wide


def pack_kernel(places, block_ref, up_ref, down_ref):
    band, width = block_ref.shape[1], block_ref.shape[2]
    half = (up_ref.shape[0] - ROWS) // 2
    lane = lax.broadcasted_iota(jnp.int32, (ROWS, width), 1)
    note = jnp.zeros((ROWS, width), jnp.int32)
    for b in range(places.shape[1]):
        for i in range(2):
            note = jnp.where(lane == 2 * b + i, places[i, b] + 1, note)
    note = note.astype(jnp.float32)
    for ch in range(2):
        up_ref[ch * half:(ch + 1) * half] = block_ref[ch, :half]
        down_ref[ch * half:(ch + 1) * half] = block_ref[ch, band - half:]
    up_ref[2 * half:] = note
    down_ref[2 * half:] = note


def weight_kernel(near, probe_ref, out_ref, total, column):
    band, width = out_ref.shape
    patch = probe_ref.shape[1]
    half = patch // 2
    last = width // LANES - patch // LANES - 1
    power = probe_ref[0] * probe_ref[0] + probe_ref[1] * probe_ref[1]
    total[...] = jnp.ones(total.shape, jnp.float32)
    for b in range(near.shape[0]):
        group = b * 3 // near.shape[0]
        top, drop = row_spot(near[b, 0])
        base, shift = column_spot(near[b, 1], last)
        term = power * near[b, 2].astype(jnp.float32)
        slot = column.at[b % 2]
        spread_rows(slot, term, top, drop)
        if group == 0:
            add_columns(total, (slice(None),), slot[half:half + band], base, shift)
        elif group == 1:
            add_columns(total, (slice(0, half),), slot[half + band:], base, shift)
        else:
            add_columns(total, (slice(band - half, band),), slot[:half], base, shift)
    out_ref[...] = 1.0 / total[...]


def gradient_kernel(places, low_ref, block_ref, high_ref, probe_ref, amp_ref, table_ref, ramp_ref,
                    up_ref, own_ref, down_ref, stat_ref, field, column):
    count, patch = amp_ref.shape[0], amp_ref.shape[1]
    half, band, width = patch // 2, block_ref.shape[1], block_ref.shape[2]
    field[:, half:half + band] = block_ref[...]
    for ch in range(2):
        field[ch, :half] = low_ref[ch * half:(ch + 1) * half]
        field[ch, half + band:] = high_ref[ch * half:(ch + 1) * half]
    own_ref[...] = jnp.zeros(own_ref.shape, jnp.float32)
    probe_real = probe_ref[0]
    probe_imag = probe_ref[1]
    window = patch + LANES
    tall = patch + ROWS
    last = (width - window) // LANES
    spots = []
    patches = []
    waves = []
    for b in range(count):
        row = places[b, 0]
        col = places[b, 1]
        top, drop = row_spot(row)
        base, shift = column_spot(col, last)
        spots.append((top, drop, base, shift))
        cut = []
        for ch in range(2):
            wide = field[ch, pl.ds(top, tall), pl.ds(base, window)]
            narrow = pltpu.roll(wide, lax.rem(window - shift, window), 1)[:, :patch]
            cut.append(pltpu.roll(narrow, lax.rem(tall - drop, tall), 0)[:patch])
        patches.append(cut)
        waves.append((probe_real * cut[0] - probe_imag * cut[1], probe_real * cut[1] + probe_imag * cut[0]))
    forward = (table_ref[0], table_ref[1])
    backward = (table_ref[2], table_ref[3])

    def by_rows(pairs):
        return jnp.concatenate([jnp.concatenate(pair, axis=1) for pair in pairs], axis=0)

    def by_columns(pairs):
        return jnp.concatenate([jnp.concatenate(pair, axis=0) for pair in pairs], axis=1)

    def from_rows(whole):
        return [(whole[b * patch:(b + 1) * patch, :patch], whole[b * patch:(b + 1) * patch, patch:]) for b in range(count)]

    def from_columns(whole):
        return [(whole[:patch, b * patch:(b + 1) * patch], whole[patch:, b * patch:(b + 1) * patch]) for b in range(count)]

    middle = from_rows(product(split_halves(by_rows(waves)), forward))
    spectra = from_columns(product(backward, split_halves(by_columns(middle))))
    fixed = []
    for b in range(count):
        real, imag = spectra[b]
        factor = amp_ref[b] / jnp.maximum(jnp.sqrt(real * real + imag * imag), 0.5)
        fixed.append((factor * real, factor * imag))
    middle = from_columns(product(forward, split_halves(by_columns(fixed))))
    back = from_rows(product(split_halves(by_rows(middle)), backward))
    numer_real = jnp.zeros((patch, patch), jnp.float32)
    numer_imag = jnp.zeros((patch, patch), jnp.float32)
    denom = jnp.zeros((patch, patch), jnp.float32)
    for b in range(count):
        top, drop, base, shift = spots[b]
        cut_real, cut_imag = patches[b]
        diff_real = back[b][0] - waves[b][0]
        diff_imag = back[b][1] - waves[b][1]
        numer_real += cut_real * diff_real + cut_imag * diff_imag
        numer_imag += cut_real * diff_imag - cut_imag * diff_real
        denom += cut_real * cut_real + cut_imag * cut_imag
        terms = (probe_real * diff_real + probe_imag * diff_imag,
                 probe_real * diff_imag - probe_imag * diff_real)
        for ch, term in enumerate(terms):
            spread_rows(column.at[ch], term, top, drop)
            up_ref[ch, b] = column[ch, :half]
            add_columns(own_ref, (ch, slice(None)), column[ch, half:half + band], base, shift)
            down_ref[ch, b] = column[ch, half + band:]
    share = stat_ref.shape[2]
    for ch, value in enumerate((numer_real, numer_imag, denom)):
        for i in range(stat_ref.shape[0]):
            stat_ref[i, ch] = value[i * share:(i + 1) * share]


def update_kernel(near, object_ref, own_ref, weight_ref, above_ref, below_ref, out_ref, imag_ref, total):
    band, width = own_ref.shape[1], own_ref.shape[2]
    count, half, patch = above_ref.shape[1], above_ref.shape[2], above_ref.shape[3]
    last = width // LANES - patch // LANES - 1
    total[...] = own_ref[...]
    for b in range(count):
        for group, ref, start in ((1, above_ref, 0), (2, below_ref, band - half)):
            base, shift = column_spot(near[group * count + b, 1], last)
            for ch in range(2):
                add_columns(total, (ch, slice(start, start + half)), ref[ch, b], base, shift)
    scale = weight_ref[...]
    out_ref[0] = object_ref[0] + total[0] * scale
    imag = object_ref[1] + total[1] * scale
    out_ref[1] = imag
    imag_ref[...] = imag


def ramp_kernel(high_ref, low_ref):
    rows, width = high_ref.shape
    line = lax.broadcasted_iota(jnp.int32, (rows, width), 0) + pl.program_id(0) * rows
    differ = line - lax.broadcasted_iota(jnp.int32, (rows, width), 1)
    spread = differ.astype(jnp.float32)
    squared = jnp.maximum(spread * spread, 1.0)
    odd_terms = jnp.where((differ & 1) != 0, (-1.0 / (math.pi * math.pi)) / squared, 0.0)
    high, low = split_halves(jnp.where(differ == 0, 0.25, odd_terms))
    high_ref[...] = high
    low_ref[...] = low


def back_kernel(sino_ref, ramp_high_ref, ramp_low_ref, index_ref, weight_ref, out_ref, parts):
    angles, rows, width = sino_ref.shape
    depth = index_ref.shape[1]
    columns = index_ref.shape[2]

    @pl.when(pl.program_id(0) == 0)
    def _():
        sino = sino_ref[...].reshape(angles * rows, width)
        filtered = product(split_halves(sino), (ramp_high_ref[...], ramp_low_ref[...])) * (math.pi / angles)
        change = pltpu.roll(filtered, width - 1, 1) - filtered
        pieces = split_halves(filtered) + split_halves(change)
        for a in range(angles):
            for i in range(4):
                parts[a, i * rows:(i + 1) * rows] = pieces[i][a * rows:(a + 1) * rows]

    bins = lax.broadcasted_iota(jnp.int32, (width, columns), 0)
    for z in range(depth):
        result = jnp.zeros((rows, columns), jnp.float32)
        for a in range(angles):
            chosen = jnp.where(bins == index_ref[a, z:z + 1, :], 1.0, 0.0).astype(jnp.bfloat16)
            got = jnp.dot(parts[a], chosen, preferred_element_type=jnp.float32)
            lower = got[:rows] + got[rows:2 * rows]
            rise = got[2 * rows:3 * rows] + got[3 * rows:]
            result += lower + weight_ref[a, z:z + 1, :] * rise
        out_ref[:, z, :] = result


def on_device(amplitude, offsets, probe_field, object_field, interp_index, interp_weight):
    f32 = jnp.float32
    band = object_field.shape[2]
    width = object_field.shape[3]
    patch = probe_field.shape[1]
    half = patch // 2
    vmem = pl.BlockSpec(memory_space=pltpu.VMEM)
    smem = pl.BlockSpec(memory_space=pltpu.SMEM)
    layer = object_field[0]
    shares = lax.axis_size("angle") * lax.axis_size("pos")
    count = offsets.shape[1]
    packed = jax.ShapeDtypeStruct((2 * half + ROWS, width), f32)
    to_above, to_below = pl.pallas_call(
        pack_kernel,
        name="pack",
        out_shape=(packed, packed),
        in_specs=[smem, vmem],
        out_specs=[vmem] * 2,
    )(offsets[0].T, layer)
    low = passed_along(to_below, "pos", 1)
    high = passed_along(to_above, "pos", -1)
    anchor = lax.axis_index("pos") * band - half
    places = offsets[0] - jnp.stack([anchor, 0]).astype(jnp.int32)
    near = [jnp.concatenate([places, jnp.ones((count, 1), jnp.int32)], axis=1)]
    for message, far in ((low, anchor - band), (high, anchor + band)):
        note = message[2 * half, :2 * count].reshape(count, 2).astype(jnp.int32)
        valid = note[:, 1:] > 0
        there = note - 1 - jnp.stack([far, 0]).astype(jnp.int32)
        near.append(jnp.concatenate([jnp.where(valid, there, 0), valid.astype(jnp.int32)], axis=1))
    near = jnp.concatenate(near, axis=0)
    ramp_rows = width // 4
    ramp_high, ramp_low = pl.pallas_call(
        ramp_kernel,
        name="ramp",
        grid=(width // ramp_rows,),
        out_shape=(jax.ShapeDtypeStruct((width, width), jnp.bfloat16),) * 2,
        out_specs=[pl.BlockSpec((ramp_rows, width), lambda i: (i, 0))] * 2,
        cost_estimate=pl.CostEstimate(flops=20 * width * width, transcendentals=0, bytes_accessed=4 * width * width),
    )()
    up, own, down, stats = pl.pallas_call(
        gradient_kernel,
        name="gradient",
        out_shape=(
            jax.ShapeDtypeStruct((2, count, half, patch), f32),
            jax.ShapeDtypeStruct((2, band, width), f32),
            jax.ShapeDtypeStruct((2, count, half, patch), f32),
            jax.ShapeDtypeStruct((shares, 3, patch // shares, patch), f32),
        ),
        in_specs=[smem] + [vmem] * 6 + [pl.BlockSpec(memory_space=pl.ANY)],
        out_specs=[vmem] * 4,
        scratch_shapes=[pltpu.VMEM((2, band + patch, width), f32), pltpu.VMEM((2, band + patch, patch), f32)],
    )(places, low, layer, high, probe_field, amplitude[0], dft_tables(patch), ramp_high)
    from_below = passed_along(up, "pos", -1)
    from_above = passed_along(down, "pos", 1)
    weight = pl.pallas_call(
        weight_kernel,
        name="weight",
        out_shape=jax.ShapeDtypeStruct((band, width), f32),
        in_specs=[smem, vmem],
        out_specs=vmem,
        scratch_shapes=[pltpu.VMEM((band, width), f32), pltpu.VMEM((2, band + patch, patch), f32)],
        cost_estimate=pl.CostEstimate(flops=20 * width * width, transcendentals=0, bytes_accessed=4 * band * width),
    )(near, probe_field)
    new_layer, imag = pl.pallas_call(
        update_kernel,
        name="update",
        out_shape=(jax.ShapeDtypeStruct((2, band, width), f32), jax.ShapeDtypeStruct((band, width), f32)),
        in_specs=[smem] + [vmem] * 5,
        out_specs=[vmem] * 2,
        scratch_shapes=[pltpu.VMEM((2, band, width), f32)],
    )(near, layer, own, weight, from_above, from_below)
    everyone = ("angle", "pos")
    angles = lax.axis_size("angle")
    regrouped = lax.all_to_all(imag.reshape(angles, band // angles, width), "angle", split_axis=0, concat_axis=0, tiled=True)
    shared = lax.all_to_all(stats, everyone, split_axis=0, concat_axis=0, tiled=True)
    mine = jnp.sum(shared, axis=0)
    step = mine[:2] / (mine[2:] + 1.0)
    copies = jnp.broadcast_to(step[None], (shares,) + step.shape)
    steps = lax.all_to_all(copies, everyone, split_axis=0, concat_axis=0, tiled=True)
    new_probe = probe_field + jnp.swapaxes(steps, 0, 1).reshape(2, patch, patch)
    rows = band // angles
    zwin = interp_index.shape[1]
    columns = min(BINS, width)
    recon = pl.pallas_call(
        back_kernel,
        name="back",
        grid=(width // columns,),
        out_shape=jax.ShapeDtypeStruct((rows, zwin, width), f32),
        in_specs=[
            pl.BlockSpec((angles, rows, width), lambda i: (0, 0, 0)),
            pl.BlockSpec((width, width), lambda i: (0, 0)),
            pl.BlockSpec((width, width), lambda i: (0, 0)),
            pl.BlockSpec((angles, zwin, columns), lambda i: (0, 0, i)),
            pl.BlockSpec((angles, zwin, columns), lambda i: (0, 0, i)),
        ],
        out_specs=pl.BlockSpec((rows, zwin, columns), lambda i: (0, 0, i)),
        scratch_shapes=[pltpu.VMEM((angles, 4 * rows, width), jnp.bfloat16)],
        compiler_params=pltpu.CompilerParams(dimension_semantics=("arbitrary",)),
    )(regrouped, ramp_high, ramp_low, interp_index, interp_weight)
    return (new_layer[None], new_probe, recon[None])


def solution(mesh):
    placed = (
        P("angle", "pos", None, None),
        P("angle", "pos", None),
        P(),
        P("angle", None, "pos", None),
        P(),
        P(),
    )

    return jax.shard_map(
        on_device,
        mesh=mesh,
        in_specs=placed,
        out_specs=(P("angle", None, "pos", None), P(), P("pos", "angle", None, None)),
        check_vma=False,
    )
```
